16 devices in a mesh: fsdp: 16 (over z, y, x, core).
Axes of the slice: x: 2, y: 2, z: 2, core: 2. Of those that a mesh axis runs over, the one named last changes fastest.
Arguments:
- left_mat: bfloat16 [65536, 2048], P('fsdp')
- right_mat: bfloat16 [2048, 2048], P('fsdp')
Outputs:
- output: bfloat16 [65536, 2048], P('fsdp')
All inputs are finite; a program needn't handle non-finite values.
Results may differ from the reference program's by a relative error of at most 0.001.
Values are sent between devices in bfloat16 or wider.
A program may use at most 1 GiB of HBM per device.

```python
import jax
import jax.numpy as jnp

ROWS_TOTAL = 65536
IN_WIDTH = 2048
OUT_WIDTH = 2048


def setup_inputs(seed: int = 0) -> dict:
    base_key = jax.random.key(seed)
    key_left, key_right = jax.random.split(base_key)
    left_vals = jax.random.normal(key_left, (ROWS_TOTAL, IN_WIDTH), jnp.float32)
    right_vals = jax.random.normal(key_right, (IN_WIDTH, OUT_WIDTH), jnp.float32) * (IN_WIDTH ** -0.5)
    return {"left_mat": left_vals.astype(jnp.bfloat16), "right_mat": right_vals.astype(jnp.bfloat16)}


def reference(left_mat, right_mat):
    return jnp.dot(left_mat, right_mat, preferred_element_type=jnp.float32).astype(jnp.bfloat16)
```

```python
import functools

import jax
import jax.numpy as jnp
from jax import lax
from jax.experimental import pallas as pl
from jax.experimental.pallas import tpu as pltpu
from jax.sharding import PartitionSpec as P

MESH = pl.DeviceIdType.MESH
CHUNKS = 4
SUB = 256
LAST = 512


def flip(index, stride):
    return index + stride - 2 * stride * lax.rem(lax.div(index, stride), 2)


def dot(a, b):
    return jnp.dot(a, b, preferred_element_type=jnp.float32)


def gather_kernel(a_hbm, b_hbm, b_all, a_all, acc, a_sem, own_sem, send_sem, recv_sem, pair_send, pair_recv, far_send, far_recv):
    me = lax.axis_index("fsdp")
    depth = b_hbm.shape[0]
    wide = b_all.shape[2]
    rows = acc.shape[1]
    half = rows // 2
    mate = flip(me, 1)
    dev_x, dev_y, dev_z = flip(me, 2), flip(me, 4), flip(me, 8)
    dev_xy, dev_yz, dev_zx = flip(dev_x, 4), flip(dev_y, 8), flip(dev_z, 2)
    dev_far = flip(dev_xy, 8)
    near = (dev_x, dev_y, dev_z)
    diag = (dev_xy, dev_yz, dev_zx)
    order = (me, *near, *diag, dev_far)

    def chip_rows(device):
        return pl.ds(pl.multiple_of(lax.div(device, 2) * (2 * depth), 2 * depth), 2 * depth)

    def block(j, device, columns=slice(None)):
        return b_all.at[j, pl.ds(pl.multiple_of(device * depth, depth), depth), columns]

    def link(kind, j, device, target):
        ref = block(j, device)
        return pltpu.make_async_remote_copy(ref, ref, send_sem.at[kind, j], recv_sem.at[kind, j], device_id=(target,), device_id_type=MESH)

    def pair(kind, j, device):
        ref = block(j, device)
        return pltpu.make_async_remote_copy(ref, ref, pair_send.at[kind, j], pair_recv.at[kind, j], device_id=(mate,), device_id_type=MESH)

    w4 = wide // 4
    pieces = ((2, 0, slice(None)), (0, 1, slice(None)), (1, 2, slice(None)),
              (2, 3, pl.ds(0, w4)), (0, 3, pl.ds(w4, w4)), (1, 3, pl.ds(2 * w4, 2 * w4)))
    carried = {2: dev_xy, 0: dev_yz, 1: dev_zx}

    def far(p, device):
        d, j, columns = pieces[p]
        ref = block(j, device, columns)
        return pltpu.make_async_remote_copy(ref, ref, far_send.at[p], far_recv.at[p], device_id=(near[d],), device_id_type=MESH)

    def a_copy(i):
        cols = chip_rows(order[i])
        return pltpu.make_async_copy(a_hbm.at[:, cols], a_all.at[:, cols], a_sem.at[i])

    def own_copy(j):
        return pltpu.make_async_copy(b_hbm.at[:, pl.ds(j * wide, wide)], block(j, me), own_sem.at[j])

    for j in range(CHUNKS):
        own_copy(j).start()
    for i in range(8):
        a_copy(i).start()

    barrier = pltpu.get_barrier_semaphore()
    for device in (mate, *near):
        pl.semaphore_signal(barrier, inc=1, device_id=(device,), device_id_type=MESH)
    pl.semaphore_wait(barrier, 4)

    for j in range(CHUNKS):
        own_copy(j).wait()
        pair(0, j, me).start()
        for kind in range(3):
            link(kind, j, me, near[kind]).start()

    onward = ((5, 2), (3, 0), (4, 1))

    def serve_near(j):
        for kind in range(3):
            link(kind, j, near[kind], near[kind]).wait_recv()
            pair(1 + kind, j, near[kind]).start()
            new_kind, d = onward[kind]
            link(new_kind, j, near[kind], near[d]).start()

    def serve_diag(j):
        for kind in range(3):
            link(3 + kind, j, diag[kind], near[kind]).wait_recv()
            pair(4 + kind, j, diag[kind]).start()

    def send_far(p):
        far(p, carried[pieces[p][0]]).start()

    def add(j, lo, hi, sources, first):
        for r in range(lo, hi, SUB):
            rs = pl.ds(r, SUB)
            total = None if first else acc[j, rs, :]
            for device in sources:
                ks = chip_rows(device)
                term = dot(a_all[rs, ks], b_all[j, ks, :])
                total = term if total is None else total + term
            acc[j, rs, :] = total

    a_copy(0).wait()

    @pl.loop(0, CHUNKS)
    def _(j):
        pair(0, j, mate).wait_recv()
        add(j, 0, rows, (me,), True)

    serve_near(0)
    for i in range(1, 8):
        a_copy(i).wait()

    @pl.loop(0, 2 * CHUNKS)
    def _(s):
        j = lax.rem(s, CHUNKS)
        phase = lax.div(s, CHUNKS)
        sources = [n + phase * (d - n) for n, d in zip(near, diag)]
        for i in range(3):
            pair(1 + 3 * phase + i, j, flip(sources[i], 1)).wait_recv()
        add(j, 0, half, sources, False)

        @pl.when(s < CHUNKS - 1)
        def _():
            serve_near(s + 1)

        @pl.when((s >= CHUNKS - 1) & (s < 2 * CHUNKS - 1))
        def _():
            serve_diag(s - (CHUNKS - 1))

        for c in range(CHUNKS):
            @pl.when(s == CHUNKS - 1 + c)
            def _():
                for p in range(6):
                    if pieces[p][1] == c:
                        send_far(p)

        add(j, half, rows, sources, False)

    for p in range(6):
        far(p, dev_far).wait_recv()
        if p < 3:
            pair(7, p, dev_far).start()
    pair(7, 3, dev_far).start()
    for j in range(CHUNKS):
        pair(7, j, flip(dev_far, 1)).wait_recv()

    for j in range(CHUNKS):
        for kind in range(3):
            link(kind, j, me, near[kind]).wait_send()
            new_kind, d = onward[kind]
            link(new_kind, j, near[kind], near[d]).wait_send()
        for i in range(8):
            pair(i, j, order[i]).wait_send()
    for p in range(6):
        far(p, carried[pieces[p][0]]).wait_send()


def finish_kernel(b_ref, a_ref, acc_ref, c_ref):
    step = pl.program_id(0)
    steps = pl.num_programs(0)
    chunks, size, wide = b_ref.shape
    rows = c_ref.shape[0]
    far = 7 - lax.div(lax.axis_index("fsdp"), 2)
    ks = pl.ds(pl.multiple_of(far * 256, 256), 256)

    @pl.when(step < steps - 1)
    def _():
        for j in range(chunks):
            for r in range(0, rows, SUB):
                rs = pl.ds(pl.multiple_of(step * rows + r, SUB), SUB)
                total = acc_ref[j, rs, :] + dot(a_ref[rs, ks], b_ref[j, ks, :])
                c_ref[pl.ds(r, SUB), j * wide:(j + 1) * wide] = total.astype(c_ref.dtype)

    @pl.when(step == steps - 1)
    def _():
        base = a_ref.shape[0] - rows
        for j in range(chunks):
            for r in range(0, rows, SUB):
                total = dot(a_ref[pl.ds(base + r, SUB), :], b_ref[j])
                c_ref[pl.ds(r, SUB), j * wide:(j + 1) * wide] = total.astype(c_ref.dtype)


def solution(mesh):
    def local(a, b):
        rows, size = a.shape
        depth, cols = b.shape
        wide = cols // CHUNKS
        main = rows - LAST
        vmem = pl.BlockSpec(memory_space=pltpu.VMEM)
        hbm = pl.BlockSpec(memory_space=pl.ANY)
        dma = pltpu.SemaphoreType.DMA
        b_all, a_all, acc = pl.pallas_call(
            gather_kernel,
            out_shape=(
                pltpu.VMEM((CHUNKS, size, wide), jnp.bfloat16),
                pltpu.VMEM((rows, size), jnp.bfloat16),
                pltpu.VMEM((CHUNKS, main, wide), jnp.float32),
            ),
            in_specs=[hbm, hbm],
            out_specs=(vmem, vmem, vmem),
            scratch_shapes=[
                dma((8,)), dma((CHUNKS,)),
                dma((6, CHUNKS)), dma((6, CHUNKS)),
                dma((8, CHUNKS)), dma((8, CHUNKS)),
                dma((6,)), dma((6,)),
            ],
            compiler_params=pltpu.CompilerParams(collective_id=0, has_side_effects=True, vmem_limit_bytes=1 << 20),
            name="gather",
        )(a, pltpu.with_memory_space_constraint(b, pltpu.HBM))
        return pl.pallas_call(
            finish_kernel,
            grid=(rows // LAST,),
            out_shape=jax.ShapeDtypeStruct((rows, cols), jnp.bfloat16),
            in_specs=[vmem, vmem, vmem],
            out_specs=pl.BlockSpec((LAST, cols), lambda i: (i, 0)),
            compiler_params=pltpu.CompilerParams(vmem_limit_bytes=8 << 20),
            name="finish",
        )(*(pltpu.with_memory_space_constraint(v, pltpu.VMEM) for v in (b_all, a_all, acc)))

    spec = P("fsdp", None)
    return jax.shard_map(local, mesh=mesh, in_specs=(spec, spec), out_specs=spec, check_vma=False)
```

```python
import jax
import jax.numpy as jnp
from jax import lax
from jax.experimental import pallas as pl
from jax.experimental.pallas import tpu as pltpu
from jax.sharding import PartitionSpec as P

MESH = pl.DeviceIdType.MESH
CHUNKS = 8
SUB = 256
LAST = 256
STAGE = 768
EARLY = 5


def flip(index, stride):
    return index + stride - 2 * stride * lax.rem(lax.div(index, stride), 2)


def dot(a, b):
    return jnp.dot(a, b, preferred_element_type=jnp.float32)


def pick(d, values):
    return jnp.where(d == 0, values[0], jnp.where(d == 1, values[1], values[2]))


def gather_kernel(a_hbm, b_hbm, b_all, a_all, acc, a_sem, own_sem, sent, near_sem, diag_sem, far_sem, pair_own, pair_near, pair_diag, pair_far):
    me = lax.axis_index("fsdp")
    depth = b_hbm.shape[0]
    wide = b_all.shape[2]
    rows = acc.shape[1]
    mate = flip(me, 1)
    dev_x, dev_y, dev_z = flip(me, 2), flip(me, 4), flip(me, 8)
    dev_xy, dev_yz, dev_zx = flip(dev_x, 4), flip(dev_y, 8), flip(dev_z, 2)
    dev_far = flip(dev_xy, 8)
    near = (dev_x, dev_y, dev_z)
    diag = (dev_xy, dev_yz, dev_zx)
    order = (me, *near, *diag, dev_far)
    split = CHUNKS - 2

    def chip_rows(device):
        return pl.ds(pl.multiple_of(lax.div(device, 2) * (2 * depth), 2 * depth), 2 * depth)

    def block(j, device, columns=slice(None)):
        return b_all.at[j, pl.ds(pl.multiple_of(device * depth, depth), depth), columns]

    def link(sem, j, device, target, columns=slice(None)):
        ref = block(j, device, columns)
        return pltpu.make_async_remote_copy(ref, ref, sent.at[0], sem, device_id=(target,), device_id_type=MESH)

    def pair(sem, j, device):
        ref = block(j, device)
        return pltpu.make_async_remote_copy(ref, ref, sent.at[1], sem, device_id=(mate,), device_id_type=MESH)

    def settle(sem, ref):
        pltpu.make_async_copy(ref, ref, sem).wait()

    shift = lax.rem(me, 2) * depth

    def three(j):
        return b_all.at[j, pl.ds(pl.multiple_of(shift, depth), 3 * depth), :]

    def across(lo, hi, device):
        return b_all.at[pl.ds(lo, hi - lo), pl.ds(pl.multiple_of(device * depth, depth), depth), :]

    def a_copy(i):
        cols = chip_rows(order[i])
        group = 0 if i == 0 else 1 if i < 4 else 2
        return pltpu.make_async_copy(a_hbm.at[:, cols], a_all.at[:, cols], a_sem.at[group])

    def a_wait(lo, hi):
        width = (hi - lo) * 2 * depth
        settle(a_sem.at[0 if lo == 0 else 1 if lo == 1 else 2], a_all.at[:, pl.ds(pl.multiple_of(shift, depth), width)])

    def own_copy(j):
        return pltpu.make_async_copy(b_hbm.at[:, pl.ds(j * wide, wide)], block(j, me), own_sem)

    for j in range(CHUNKS):
        own_copy(j).start()
    a_copy(0).start()

    barrier = pltpu.get_barrier_semaphore()
    for device in (mate, *near):
        pl.semaphore_signal(barrier, inc=1, device_id=(device,), device_id_type=MESH)
    pl.semaphore_wait(barrier, 4)

    settle(own_sem, across(0, CHUNKS, me))
    for j in range(CHUNKS):
        for kind in range(3):
            link(near_sem.at[j], j, me, near[kind]).start()
        pair(pair_own.at[0 if j < EARLY else 1], j, me).start()
    for i in range(1, 4):
        a_copy(i).start()

    def serve_near(j):
        settle(near_sem.at[j], three(j))
        for kind, d in enumerate((2, 0, 1)):
            pair(pair_near.at[j], j, near[kind]).start()
            link(diag_sem.at[j], j, near[kind], near[d]).start()

    half = wide // 2
    halves = (pl.ds(0, half), pl.ds(half, half))

    def send_far(j):
        if isinstance(j, int):
            if j == split:
                link(far_sem.at[1], j, dev_xy, dev_z, halves[0]).start()
                link(far_sem.at[1], j, dev_yz, dev_x, halves[1]).start()
                return
            d = min(j // 2, 2)
            source, target = (dev_xy, dev_yz, dev_zx)[d], (dev_z, dev_x, dev_y)[d]
        else:
            d = lax.div(j, 2)
            source, target = pick(d, (dev_xy, dev_yz, dev_zx)), pick(d, (dev_z, dev_x, dev_y))
        link(far_sem.at[0 if not isinstance(j, int) or j < split else 1], j, source, target).start()

    def serve_diag(j):
        settle(diag_sem.at[j], three(j))
        send_far(j)
        for kind in range(3):
            pair(pair_diag.at[j], j, diag[kind]).start()

    def serve_far(group):
        lo, hi = ((0, split), (split, CHUNKS))[group]
        settle(far_sem.at[group], across(lo, hi, dev_far))
        for j in range(lo, hi):
            pair(pair_far, j, dev_far).start()

    def add(j, sources, first=False):
        for r in range(0, rows, SUB):
            rs = pl.ds(r, SUB)
            total = None if first else acc[j, rs, :]
            for device in sources:
                ks = chip_rows(device)
                term = dot(a_all[rs, ks], b_all[j, ks, :])
                total = term if total is None else total + term
            acc[j, rs, :] = total

    a_wait(0, 1)
    settle(pair_own.at[0], across(0, EARLY, mate))
    for j in range(EARLY):
        add(j, (me,), True)
    serve_near(0)
    for i in range(4, 8):
        a_copy(i).start()
    settle(pair_own.at[1], across(EARLY, CHUNKS, mate))
    for j in range(EARLY, CHUNKS):
        add(j, (me,), True)

    def steps(phase, lo, hi, serve):
        @pl.loop(lo + phase * CHUNKS, hi + phase * CHUNKS)
        def _(s):
            j = lax.rem(s, CHUNKS)
            late = lax.div(s, CHUNKS)
            serve(j)
            sources = [n + late * (d - n) for n, d in zip(near, diag)]
            settle((pair_diag if phase else pair_near).at[j], three(j))
            add(j, sources)

    def plan(table):
        def serve(j):
            for k, parts in table.items():
                @pl.when(j == k)
                def _():
                    for part, arg in parts:
                        part(arg)
        return serve

    a_wait(1, 4)
    steps(0, 0, 6, lambda j: serve_near(j + 1))
    steps(0, 6, 8, plan({6: ((serve_near, 7), (serve_diag, 0)), 7: ((serve_diag, 1),)}))
    a_wait(4, 8)
    steps(1, 0, 2, plan({0: ((serve_diag, 2),), 1: ((serve_diag, 3), (serve_diag, 4))}))
    steps(1, 2, 4, plan({2: ((serve_diag, 5),), 3: ((serve_diag, 6),)}))
    steps(1, 4, 6, plan({4: ((serve_diag, 7),)}))
    steps(1, 6, 8, plan({6: ((serve_far, 0),), 7: ((serve_far, 1),)}))

    settle(pair_far, across(0, CHUNKS, flip(dev_far, 1)))
    settle(sent.at[0], b_all.at[pl.ds(0, CHUNKS - 1), pl.ds(0, 8 * depth), :])
    settle(sent.at[1], b_all.at[:, pl.ds(0, 8 * depth), :])


def finish_kernel(b_ref, a_ref, acc_ref, c_hbm, stage, sem):
    chunks, size, wide = b_ref.shape
    main = acc_ref.shape[1]
    blocks = main // STAGE
    last = c_hbm.shape[0] - main
    depth = size // 8
    far = 7 - lax.div(lax.axis_index("fsdp"), 2)
    ks = pl.ds(pl.multiple_of(far * depth, depth), depth)

    def put(i):
        rs = pl.ds(pl.multiple_of(i * STAGE, STAGE), STAGE)
        slot = lax.rem(i, 2)
        return pltpu.make_async_copy(stage.at[slot], c_hbm.at[rs, :], sem.at[slot])

    @pl.loop(0, blocks)
    def _(i):
        @pl.when(i >= 2)
        def _():
            put(i - 2).wait()

        slot = lax.rem(i, 2)
        for j in range(chunks):
            for r in range(0, STAGE, SUB):
                rs = pl.ds(pl.multiple_of(i * STAGE + r, SUB), SUB)
                total = acc_ref[j, rs, :] + dot(a_ref[rs, ks], b_ref[j, ks, :])
                stage[slot, pl.ds(r, SUB), j * wide:(j + 1) * wide] = total.astype(stage.dtype)
        put(i).start()

    put(blocks - 2).wait()
    slot = blocks % 2
    for j in range(chunks):
        for r in range(0, last, SUB):
            total = dot(a_ref[pl.ds(main + r, SUB), :], b_ref[j])
            stage[slot, pl.ds(r, SUB), j * wide:(j + 1) * wide] = total.astype(stage.dtype)
    tail = pltpu.make_async_copy(stage.at[slot, pl.ds(0, last)], c_hbm.at[pl.ds(main, last), :], sem.at[slot])
    tail.start()
    put(blocks - 1).wait()
    tail.wait()


def solution(mesh):
    def local(a, b):
        rows, size = a.shape
        depth, cols = b.shape
        wide = cols // CHUNKS
        main = rows - LAST
        vmem = pl.BlockSpec(memory_space=pltpu.VMEM)
        hbm = pl.BlockSpec(memory_space=pl.ANY)
        dma = pltpu.SemaphoreType.DMA
        parts = pl.pallas_call(
            gather_kernel,
            out_shape=(
                pltpu.VMEM((CHUNKS, size, wide), jnp.bfloat16),
                pltpu.VMEM((rows, size), jnp.bfloat16),
                pltpu.VMEM((CHUNKS, main, wide), jnp.float32),
            ),
            in_specs=[hbm, hbm],
            out_specs=(vmem, vmem, vmem),
            scratch_shapes=[
                dma((3,)), dma, dma((2,)),
                dma((CHUNKS,)), dma((CHUNKS,)), dma((2,)),
                dma((2,)), dma((CHUNKS,)), dma((CHUNKS,)), dma,
            ],
            compiler_params=pltpu.CompilerParams(collective_id=0, has_side_effects=True, vmem_limit_bytes=1 << 20),
            name="gather",
        )(a, pltpu.with_memory_space_constraint(b, pltpu.HBM))
        return pl.pallas_call(
            finish_kernel,
            out_shape=jax.ShapeDtypeStruct((rows, cols), jnp.bfloat16),
            in_specs=[vmem, vmem, vmem],
            out_specs=hbm,
            scratch_shapes=[pltpu.VMEM((2, STAGE, cols), jnp.bfloat16), dma((2,))],
            compiler_params=pltpu.CompilerParams(vmem_limit_bytes=7 << 20),
            name="finish",
        )(*(pltpu.with_memory_space_constraint(v, pltpu.VMEM) for v in parts))

    spec = P("fsdp", None)
    return jax.shard_map(local, mesh=mesh, in_specs=(spec, spec), out_specs=spec, check_vma=False)
```

```python
import jax
import jax.numpy as jnp
from jax import lax
from jax.experimental import pallas as pl
from jax.experimental.pallas import tpu as pltpu
from jax.sharding import PartitionSpec as P

MESH = pl.DeviceIdType.MESH
CHUNKS = 8
SUB = 512
TILE = 256
SLOTS = 4
LEFT = 2
EARLY = 5


def flip(index, stride):
    return index + stride - 2 * stride * lax.rem(lax.div(index, stride), 2)


def dot(a, b):
    return jnp.dot(a, b, preferred_element_type=jnp.float32)


UNITS = 2
RING = 4
LAG = 2


def accumulators():
    return [pltpu.ACC(q)((TILE, TILE), jnp.float32) for q in range(UNITS) for _ in range(RING)]


def stage_right(right, n):
    for q in range(UNITS):
        pltpu.matmul_push_rhs(right(n, q), staging_register=n % 2, mxu_index=q)


def result(tiles, i, q):
    return pltpu.matmul_pop(tiles[q * RING + i % RING])


def pick(d, values):
    return jnp.where(d == 0, values[0], jnp.where(d == 1, values[1], values[2]))


def gather_kernel(a_hbm, b_hbm, b_all, a_all, acc, a_sem, own_sem, sent, near_sem, diag_sem, far_sem, pair_own, pair_near, pair_diag, pair_far):
    me = lax.axis_index("fsdp")
    depth = b_hbm.shape[0]
    wide = b_all.shape[2]
    rows = acc.shape[1]
    mate = flip(me, 1)
    dev_x, dev_y, dev_z = flip(me, 2), flip(me, 4), flip(me, 8)
    dev_xy, dev_yz, dev_zx = flip(dev_x, 4), flip(dev_y, 8), flip(dev_z, 2)
    dev_far = flip(dev_xy, 8)
    near = (dev_x, dev_y, dev_z)
    diag = (dev_xy, dev_yz, dev_zx)
    order = (me, *near, *diag, dev_far)

    def chip_rows(device):
        return pl.ds(pl.multiple_of(lax.div(device, 2) * (2 * depth), 2 * depth), 2 * depth)

    def block(j, device, start=0, count=None):
        return b_all.at[j, pl.ds(pl.multiple_of(device * depth + start, 16), count or depth), :]

    def link(sem, j, device, target, start=0, count=None):
        ref = block(j, device, start, count)
        return pltpu.make_async_remote_copy(ref, ref, sent.at[0], sem, device_id=(target,), device_id_type=MESH)

    def pair(sem, j, device):
        ref = block(j, device)
        return pltpu.make_async_remote_copy(ref, ref, sent.at[1], sem, device_id=(mate,), device_id_type=MESH)

    def settle(sem, ref):
        pltpu.make_async_copy(ref, ref, sem).wait()

    shift = lax.rem(me, 2) * depth

    def three(j):
        return b_all.at[j, pl.ds(pl.multiple_of(shift, depth), 3 * depth), :]

    def across(lo, hi, device):
        return b_all.at[pl.ds(lo, hi - lo), pl.ds(pl.multiple_of(device * depth, depth), depth), :]

    def a_copy(i):
        cols = chip_rows(order[i])
        group = 0 if i == 0 else 1 if i < 4 else 2
        return pltpu.make_async_copy(a_hbm.at[:, cols], a_all.at[:, cols], a_sem.at[group])

    def a_wait(lo, hi):
        width = (hi - lo) * 2 * depth
        settle(a_sem.at[0 if lo == 0 else 1 if lo == 1 else 2], a_all.at[:, pl.ds(pl.multiple_of(shift, depth), width)])

    def own_copy(j):
        return pltpu.make_async_copy(b_hbm.at[:, pl.ds(j * wide, wide)], block(j, me), own_sem)

    for j in range(CHUNKS):
        own_copy(j).start()
    a_copy(0).start()

    barrier = pltpu.get_barrier_semaphore()
    for device in (mate, *near):
        pl.semaphore_signal(barrier, inc=1, device_id=(device,), device_id_type=MESH)
    pl.semaphore_wait(barrier, 4)

    settle(own_sem, across(0, CHUNKS, me))
    for j in range(CHUNKS):
        for kind in range(3):
            link(near_sem.at[j], j, me, near[kind]).start()
        pair(pair_own.at[0 if j < EARLY else 1], j, me).start()
    for i in range(1, 4):
        a_copy(i).start()

    def serve_near(j):
        settle(near_sem.at[j], three(j))
        for kind, d in enumerate((2, 0, 1)):
            pair(pair_near.at[j], j, near[kind]).start()
            link(diag_sem.at[j], j, near[kind], near[d]).start()

    part_rows = ((48, 48, 32), (32, 48, 48), (48, 32, 48))

    def send_far(j):
        start = 0
        for d, count in enumerate(part_rows[j % 3]):
            source, target = ((dev_xy, dev_z), (dev_yz, dev_x), (dev_zx, dev_y))[d]
            link(far_sem, j, source, target, start, count).start()
            start += count

    def serve_diag(j):
        settle(diag_sem.at[j], three(j))
        send_far(j)
        for kind in range(3):
            pair(pair_diag.at[j], j, diag[kind]).start()

    def serve_far():
        settle(far_sem, across(0, CHUNKS, dev_far))
        for j in range(CHUNKS):
            pair(pair_far, j, dev_far).start()

    def add(j, sources, first=False, count=1):
        for r in range(0, rows, SUB):
            rs = pl.ds(r, SUB)
            for c in range(count):
                total = None if first else acc[j + c, rs, :]
                for device in sources:
                    ks = chip_rows(device)
                    term = dot(a_all[rs, ks], b_all[j + c, ks, :])
                    total = term if total is None else total + term
                acc[j + c, rs, :] = total

    a_wait(0, 1)
    settle(pair_own.at[0], across(0, EARLY, mate))
    for j in range(EARLY):
        add(j, (me,), True)
    serve_near(0)
    for i in range(4, 8):
        a_copy(i).start()
    settle(pair_own.at[1], across(EARLY, CHUNKS, mate))
    for j in range(EARLY, CHUNKS):
        add(j, (me,), True)

    def steps(phase, lo, hi, serve, count=1):
        @pl.loop(0, (hi - lo) // count)
        def _(s):
            j = lo + s * count
            late = lax.div(j + phase * CHUNKS, CHUNKS)
            serve(j)
            sources = [n + late * (d - n) for n, d in zip(near, diag)]
            for c in range(count):
                settle((pair_diag if phase else pair_near).at[j + c], three(j + c))
            add(j, sources, False, count)

    def plan(table):
        def serve(j):
            for k, parts in table.items():
                @pl.when(j == k)
                def _():
                    for part, arg in parts:
                        part(arg)
        return serve

    a_wait(1, 4)
    steps(0, 0, 4, plan({0: ((serve_near, 1),), 1: ((serve_near, 2),), 2: ((serve_near, 3),), 3: ((serve_near, 4), (serve_near, 5))}))
    steps(0, 4, 6, plan({4: ((serve_near, 6),)}), 2)
    steps(0, 6, 8, plan({6: ((serve_near, 7), (serve_diag, 0)), 7: ((serve_diag, 1), (serve_diag, 2))}))
    a_wait(4, 8)
    steps(1, 0, 2, plan({0: ((serve_diag, 3),)}), 2)
    steps(1, 2, 3, plan({2: ((serve_diag, 4), (serve_diag, 5))}))
    steps(1, 3, 5, plan({3: ((serve_diag, 6), (serve_diag, 7))}), 2)
    steps(1, 5, 6, lambda j: serve_far())

    for j in range(CHUNKS - LEFT, CHUNKS):
        settle(pair_diag.at[j], three(j))
    settle(pair_far, across(0, CHUNKS, flip(dev_far, 1)))
    settle(sent.at[0], b_all.at[pl.ds(0, CHUNKS - 1), pl.ds(0, 8 * depth), :])
    settle(sent.at[1], b_all.at[:, pl.ds(0, 8 * depth), :])


def finish_kernel(*refs):
    pl.run_scoped(lambda *tiles: finish_body(tiles, *refs), *accumulators())


def finish_body(tiles, b_ref, a_ref, acc_ref, c_hbm, stage, sem):
    chunks, size, wide = b_ref.shape
    blocks = c_hbm.shape[0] // TILE
    count = chunks // UNITS
    depth = size // 8
    chip = lax.div(lax.axis_index("fsdp"), 2)
    far = 7 - chip
    chips = (far, flip(far, 1), flip(far, 2), flip(far, 4))

    def part(device):
        return pl.ds(pl.multiple_of(device * depth, depth), depth)

    def rows_of(b):
        return pl.ds(pl.multiple_of(b * TILE, TILE), TILE)

    def put(b):
        slot = lax.rem(b, SLOTS)
        return pltpu.make_async_copy(stage.at[slot], c_hbm.at[rows_of(b), :], sem.at[slot])

    def keep(b, slot, i):
        for q in range(UNITS):
            j = UNITS * i + q
            total = acc_ref[j, rows_of(b), :] + result(tiles, i, q)
            stage[slot, :, j * wide:(j + 1) * wide] = total.astype(stage.dtype)

    passes = [(i, d) for i in range(count) for d in chips[:1 if UNITS * i < chunks - LEFT else 4]]

    def right(n, q):
        i, d = passes[n]
        return b_ref[UNITS * i + q, part(d), :]

    stage_right(right, 0)

    def work(b, start=True, wait=True):
        before = b - 1 if start else 0
        for n, (i, d) in enumerate(passes):
            if n + 1 < len(passes):
                stage_right(right, n + 1)
            for q in range(UNITS):
                pltpu.matmul_acc_lhs(tiles[q * RING + i % RING], a_ref[rows_of(b), part(d)], load_staged_rhs=n % 2)
            if n + 1 == len(passes):
                stage_right(right, 0)
            elif passes[n + 1][0] == i:
                continue
            if i < LAG:
                keep(before, lax.rem(b + SLOTS - 1, SLOTS), count - LAG + i)
            else:
                keep(b, lax.rem(b, SLOTS), i - LAG)
            if i == LAG - 1:
                if start:
                    put(b - 1).start()
                if wait:
                    put(b - SLOTS).wait()

    work(0, False, False)
    pl.loop(1, SLOTS)(lambda b: work(b, True, False))
    pl.loop(SLOTS, blocks)(work)
    for i in range(count - LAG, count):
        keep(blocks - 1, (blocks - 1) % SLOTS, i)
    put(blocks - 1).start()
    for q in range(UNITS):
        pltpu.matmul_acc_lhs(tiles[q * RING], a_ref[rows_of(0), part(far)], load_staged_rhs=0)
        result(tiles, 0, q)
    for b in range(blocks - SLOTS, blocks):
        put(b).wait()


def solution(mesh):
    def local(a, b):
        rows, size = a.shape
        depth, cols = b.shape
        wide = cols // CHUNKS
        vmem = pl.BlockSpec(memory_space=pltpu.VMEM)
        hbm = pl.BlockSpec(memory_space=pl.ANY)
        dma = pltpu.SemaphoreType.DMA
        parts = pl.pallas_call(
            gather_kernel,
            out_shape=(
                pltpu.VMEM((CHUNKS, size, wide), jnp.bfloat16),
                pltpu.VMEM((rows, size), jnp.bfloat16),
                pltpu.VMEM((CHUNKS, rows, wide), jnp.float32),
            ),
            in_specs=[hbm, hbm],
            out_specs=(vmem, vmem, vmem),
            scratch_shapes=[
                dma((3,)), dma, dma((2,)),
                dma((CHUNKS,)), dma((CHUNKS,)), dma,
                dma((2,)), dma((CHUNKS,)), dma((CHUNKS,)), dma,
            ],
            compiler_params=pltpu.CompilerParams(collective_id=0, has_side_effects=True, vmem_limit_bytes=7 << 20),
            name="gather",
        )(a, pltpu.with_memory_space_constraint(b, pltpu.HBM))
        return pl.pallas_call(
            finish_kernel,
            out_shape=jax.ShapeDtypeStruct((rows, cols), jnp.bfloat16),
            in_specs=[vmem, vmem, vmem],
            out_specs=hbm,
            scratch_shapes=[pltpu.VMEM((SLOTS, TILE, cols), jnp.bfloat16), dma((SLOTS,))],
            compiler_params=pltpu.CompilerParams(vmem_limit_bytes=7 << 20),
            name="finish",
        )(*(pltpu.with_memory_space_constraint(v, pltpu.VMEM) for v in parts))

    spec = P("fsdp", None)
    return jax.shard_map(local, mesh=mesh, in_specs=(spec, spec), out_specs=spec, check_vma=False)
```

```python
import jax
import jax.numpy as jnp
from jax import lax
from jax.experimental import pallas as pl
from jax.experimental.pallas import tpu as pltpu
from jax.sharding import PartitionSpec as P

MESH = pl.DeviceIdType.MESH
CHUNKS = 8
SUB = 1024
TILE = 256
BLOCK = 512
SLOTS = 3
LEFT = 2
EARLY = 5
NEAR = ((0, 1), (1, 1), (2, 1), (3, 1), (4, 2), (6, 2))


def flip(index, stride):
    return index + stride - 2 * stride * lax.rem(lax.div(index, stride), 2)


def dot(a, b):
    return jnp.dot(a, b, preferred_element_type=jnp.float32)


UNITS = 2
RING = 4
LAG = 2


def accumulators():
    return [pltpu.ACC(q)((TILE, TILE), jnp.float32) for q in range(UNITS) for _ in range(RING)]


def stage_right(right, n):
    for q in range(UNITS):
        pltpu.matmul_push_rhs(right(n, q), staging_register=n % 2, mxu_index=q)


def result(tiles, i, q):
    return pltpu.matmul_pop(tiles[q * RING + i % RING])


def pick(d, values):
    return jnp.where(d == 0, values[0], jnp.where(d == 1, values[1], values[2]))


def gather_kernel(a_hbm, b_hbm, b_all, a_all, acc, a_sem, own_sem, sent, near_sem, diag_sem, far_sem, pair_own, pair_near, pair_diag, pair_far):
    me = lax.axis_index("fsdp")
    depth = b_hbm.shape[0]
    wide = b_all.shape[2]
    rows = acc.shape[1]
    mate = flip(me, 1)
    dev_x, dev_y, dev_z = flip(me, 2), flip(me, 4), flip(me, 8)
    dev_xy, dev_yz, dev_zx = flip(dev_x, 4), flip(dev_y, 8), flip(dev_z, 2)
    dev_far = flip(dev_xy, 8)
    near = (dev_x, dev_y, dev_z)
    diag = (dev_xy, dev_yz, dev_zx)
    order = (me, *near, *diag, dev_far)

    def chip_rows(device):
        return pl.ds(pl.multiple_of(lax.div(device, 2) * (2 * depth), 2 * depth), 2 * depth)

    def block(j, device, n=1, start=0, count=None):
        return b_all.at[pl.ds(j, n), pl.ds(pl.multiple_of(device * depth + start, 16), count or depth), :]

    def link(sem, ref, target):
        return pltpu.make_async_remote_copy(ref, ref, sent.at[0], sem, device_id=(target,), device_id_type=MESH)

    def pair(sem, ref):
        return pltpu.make_async_remote_copy(ref, ref, sent.at[1], sem, device_id=(mate,), device_id_type=MESH)

    def settle(sem, ref):
        pltpu.make_async_copy(ref, ref, sem).wait()

    shift = lax.rem(me, 2) * depth

    def three(j, n=1):
        return b_all.at[pl.ds(j, n), pl.ds(pl.multiple_of(shift, depth), 3 * depth), :]

    def across(lo, hi, device):
        return b_all.at[pl.ds(lo, hi - lo), pl.ds(pl.multiple_of(device * depth, depth), depth), :]

    def a_copy(i):
        cols = chip_rows(order[i])
        group = 0 if i == 0 else 1 if i < 4 else 2
        return pltpu.make_async_copy(a_hbm.at[:, cols], a_all.at[:, cols], a_sem.at[group])

    def a_wait(lo, hi):
        width = (hi - lo) * 2 * depth
        settle(a_sem.at[0 if lo == 0 else 1 if lo == 1 else 2], a_all.at[:, pl.ds(pl.multiple_of(shift, depth), width)])

    def own_copy(j):
        return pltpu.make_async_copy(b_hbm.at[:, pl.ds(j * wide, wide)], b_all.at[j, pl.ds(pl.multiple_of(me * depth, depth), depth), :], own_sem)

    for j in range(CHUNKS):
        own_copy(j).start()
    a_copy(0).start()

    barrier = pltpu.get_barrier_semaphore()
    for device in (mate, *near):
        pl.semaphore_signal(barrier, inc=1, device_id=(device,), device_id_type=MESH)
    pl.semaphore_wait(barrier, 4)

    settle(own_sem, across(0, CHUNKS, me))
    for group, (lo, hi) in enumerate(((0, EARLY), (EARLY, CHUNKS))):
        pair(pair_own.at[group], across(lo, hi, me)).start()
    for u, (j, n) in enumerate(NEAR):
        for kind in range(3):
            link(near_sem.at[u], block(j, me, n), near[kind]).start()
    for i in range(1, 4):
        a_copy(i).start()

    def serve_near(u):
        j, n = NEAR[u]
        settle(near_sem.at[u], three(j, n))
        for kind, d in enumerate((2, 0, 1)):
            link(diag_sem.at[j // 2], block(j, near[kind], n), near[d]).start()
        for kind in range(3):
            pair(pair_near.at[u], block(j, near[kind], n)).start()

    part_rows = ((48, 48, 32), (32, 48, 48), (48, 32, 48))

    def serve_diag(u):
        settle(diag_sem.at[u], three(2 * u, 2))
        start = 0
        for d, count in enumerate(part_rows[u % 3]):
            source, target = ((dev_xy, dev_z), (dev_yz, dev_x), (dev_zx, dev_y))[d]
            link(far_sem, block(2 * u, source, 2, start, count), target).start()
            start += count
        for kind in range(3):
            pair(pair_diag.at[u], block(2 * u, diag[kind], 2)).start()

    def serve_far():
        settle(far_sem, across(0, CHUNKS, dev_far))
        pair(pair_far, across(0, CHUNKS, dev_far)).start()

    def add(j, sources, first=False, count=1):
        for r in range(0, rows, SUB):
            rs = pl.ds(r, SUB)
            for c in range(count):
                total = None if first else acc[j + c, rs, :]
                for device in sources:
                    ks = chip_rows(device)
                    term = dot(a_all[rs, ks], b_all[j + c, ks, :])
                    total = term if total is None else total + term
                acc[j + c, rs, :] = total

    a_wait(0, 1)
    settle(pair_own.at[0], across(0, EARLY, mate))
    for j in range(EARLY):
        add(j, (me,), True)
    serve_near(0)
    for i in range(4, 8):
        a_copy(i).start()
    settle(pair_own.at[1], across(EARLY, CHUNKS, mate))
    for j in range(EARLY, CHUNKS):
        add(j, (me,), True)

    def got_near(u):
        settle(pair_near.at[u], three(*NEAR[u]))

    def got_diag(u):
        settle(pair_diag.at[u], three(2 * u, 2))

    def steps(phase, lo, hi, table, count=1):
        @pl.loop(0, (hi - lo) // count)
        def _(s):
            j = lo + s * count
            late = lax.div(j + phase * CHUNKS, CHUNKS)
            for k, parts in table.items():
                @pl.when(j == k)
                def _():
                    for part, *arg in parts:
                        part(*arg)
            add(j, [n + late * (d - n) for n, d in zip(near, diag)], False, count)

    a_wait(1, 4)
    steps(0, 0, 4, {0: ((serve_near, 1), (got_near, 0)), 1: ((serve_near, 2), (got_near, 1)), 2: ((serve_near, 3), (got_near, 2)), 3: ((serve_near, 4), (got_near, 3))})
    steps(0, 4, 6, {4: ((got_near, 4),), 5: ((serve_near, 5),)})
    steps(0, 6, 8, {6: ((serve_diag, 0), (got_near, 5))}, 2)
    a_wait(4, 8)
    steps(1, 0, 2, {0: ((serve_diag, 1), (got_diag, 0))}, 2)
    steps(1, 2, 3, {2: ((serve_diag, 2), (got_diag, 1))})
    steps(1, 3, 5, {3: ((serve_diag, 3), (got_diag, 2))}, 2)
    steps(1, 5, 6, {5: ((serve_far,),)})
    got_diag(3)
    settle(pair_far, across(0, CHUNKS, flip(dev_far, 1)))
    settle(sent.at[0], b_all.at[pl.ds(0, CHUNKS - 1), pl.ds(0, 8 * depth), :])
    settle(sent.at[1], b_all.at[:, pl.ds(0, 8 * depth), :])


def finish_kernel(*refs):
    pl.run_scoped(lambda *tiles: finish_body(tiles, *refs), *accumulators())


def finish_body(tiles, b_ref, a_ref, acc_ref, c_hbm, stage, sem):
    chunks, size, wide = b_ref.shape
    blocks = c_hbm.shape[0] // BLOCK
    count = chunks // UNITS
    depth = size // 8
    chip = lax.div(lax.axis_index("fsdp"), 2)
    far = 7 - chip
    chips = (far, flip(far, 1), flip(far, 2), flip(far, 4))

    def part(device):
        return pl.ds(pl.multiple_of(device * depth, depth), depth)

    halves = BLOCK // TILE

    def rows_of(b, h=0, size=TILE):
        return pl.ds(pl.multiple_of(b * BLOCK + h * TILE, TILE), size)

    def put(b):
        slot = lax.rem(b, SLOTS)
        return pltpu.make_async_copy(stage.at[slot], c_hbm.at[rows_of(b, 0, BLOCK), :], sem.at[slot])

    def put_half(b, h):
        source = stage.at[b % SLOTS, pl.ds(h * TILE, TILE), :]
        return pltpu.make_async_copy(source, c_hbm.at[rows_of(b, h), :], sem.at[b % SLOTS if h == 0 else SLOTS])

    def keep(b, slot, t):
        h, i = divmod(t, count)
        for q in range(UNITS):
            j = UNITS * i + q
            total = acc_ref[j, rows_of(b, h), :] + result(tiles, t, q)
            stage[slot, pl.ds(h * TILE, TILE), j * wide:(j + 1) * wide] = total.astype(stage.dtype)

    passes = [(h * count + i, d) for h in range(halves) for i in range(count) for d in chips[:1 if UNITS * i < chunks - LEFT else 4]]
    every = halves * count

    def right(n, q):
        t, d = passes[n]
        return b_ref[UNITS * (t % count) + q, part(d), :]

    stage_right(right, 0)

    def work(b, start=True, wait=True, final=False):
        before = b - 1 if start else 0
        for n, (t, d) in enumerate(passes):
            if n + 1 < len(passes):
                stage_right(right, n + 1)
            for q in range(UNITS):
                pltpu.matmul_acc_lhs(tiles[q * RING + t % RING], a_ref[rows_of(b, t // count), part(d)], load_staged_rhs=n % 2)
            if n + 1 == len(passes):
                if not final:
                    stage_right(right, 0)
            elif passes[n + 1][0] == t:
                continue
            if t < LAG:
                keep(before, lax.rem(b + SLOTS - 1, SLOTS), every - LAG + t)
            else:
                keep(b, lax.rem(b, SLOTS), t - LAG)
            if t == LAG - 1:
                if start:
                    put(b - 1).start()
                if wait:
                    put(b - SLOTS).wait()
            if final and t == count + LAG - 1:
                put_half(b, 0).start()

    last = blocks - 1
    work(0, False, False)
    pl.loop(1, SLOTS)(lambda b: work(b, True, False))
    pl.loop(SLOTS, last)(work)
    work(last, True, True, True)
    for t in range(every - LAG, every):
        keep(last, last % SLOTS, t)
    put_half(last, 1).start()
    for b in range(blocks - SLOTS, last):
        put(b).wait()
    for h in range(halves):
        put_half(last, h).wait()


def solution(mesh):
    def local(a, b):
        rows, size = a.shape
        depth, cols = b.shape
        wide = cols // CHUNKS
        vmem = pl.BlockSpec(memory_space=pltpu.VMEM)
        hbm = pl.BlockSpec(memory_space=pl.ANY)
        dma = pltpu.SemaphoreType.DMA
        parts = pl.pallas_call(
            gather_kernel,
            out_shape=(
                pltpu.VMEM((CHUNKS, size, wide), jnp.bfloat16),
                pltpu.VMEM((rows, size), jnp.bfloat16),
                pltpu.VMEM((CHUNKS, rows, wide), jnp.float32),
            ),
            in_specs=[hbm, hbm],
            out_specs=(vmem, vmem, vmem),
            scratch_shapes=[
                dma((3,)), dma, dma((2,)),
                dma((len(NEAR),)), dma((CHUNKS // 2,)), dma,
                dma((2,)), dma((len(NEAR),)), dma((CHUNKS // 2,)), dma,
            ],
            compiler_params=pltpu.CompilerParams(collective_id=0, has_side_effects=True, vmem_limit_bytes=7 << 20),
            name="gather",
        )(a, pltpu.with_memory_space_constraint(b, pltpu.HBM))
        return pl.pallas_call(
            finish_kernel,
            out_shape=jax.ShapeDtypeStruct((rows, cols), jnp.bfloat16),
            in_specs=[vmem, vmem, vmem],
            out_specs=hbm,
            scratch_shapes=[pltpu.VMEM((SLOTS, BLOCK, cols), jnp.bfloat16), dma((SLOTS + 1,))],
            compiler_params=pltpu.CompilerParams(vmem_limit_bytes=15 << 19),
            name="finish",
        )(*(pltpu.with_memory_space_constraint(v, pltpu.VMEM) for v in parts))

    spec = P("fsdp", None)
    return jax.shard_map(local, mesh=mesh, in_specs=(spec, spec), out_specs=spec, check_vma=False)
```

```python
import jax
import jax.numpy as jnp
from jax import lax
from jax.experimental import pallas as pl
from jax.experimental.pallas import tpu as pltpu
from jax.sharding import PartitionSpec as P

MESH = pl.DeviceIdType.MESH
CHUNKS = 8
SUB = 1024
TILE = 256
BLOCK = 512
SLOTS = 3
LEFT = 2
EARLY = 5
NEAR = ((0, 1), (1, 1), (2, 1), (3, 1), (4, 2), (6, 2))


def flip(index, stride):
    return index + stride - 2 * stride * lax.rem(lax.div(index, stride), 2)


def dot(a, b):
    return jnp.dot(a, b, preferred_element_type=jnp.float32)


UNITS = 2
RING = 4
LAG = 3


def accumulators():
    return [pltpu.ACC(q)((TILE, TILE), jnp.float32) for q in range(UNITS) for _ in range(RING)]


def stage_right(right, n):
    for q in range(UNITS):
        pltpu.matmul_push_rhs(right(n, q), staging_register=n % 2, mxu_index=q)


def result(tiles, i, q):
    return pltpu.matmul_pop(tiles[q * RING + i % RING])


def pick(d, values):
    return jnp.where(d == 0, values[0], jnp.where(d == 1, values[1], values[2]))


def gather_kernel(a_hbm, b_hbm, b_all, a_all, acc, a_sem, own_sem, sent, near_sem, diag_sem, far_sem, pair_own, pair_near, pair_diag, pair_far):
    me = lax.axis_index("fsdp")
    depth = b_hbm.shape[0]
    wide = b_all.shape[2]
    rows = acc.shape[1]
    mate = flip(me, 1)
    dev_x, dev_y, dev_z = flip(me, 2), flip(me, 4), flip(me, 8)
    dev_xy, dev_yz, dev_zx = flip(dev_x, 4), flip(dev_y, 8), flip(dev_z, 2)
    dev_far = flip(dev_xy, 8)
    near = (dev_x, dev_y, dev_z)
    diag = (dev_xy, dev_yz, dev_zx)
    order = (me, *near, *diag, dev_far)

    def chip_rows(device):
        return pl.ds(pl.multiple_of(lax.div(device, 2) * (2 * depth), 2 * depth), 2 * depth)

    def block(j, device, n=1, start=0, count=None):
        return b_all.at[pl.ds(j, n), pl.ds(pl.multiple_of(device * depth + start, 16), count or depth), :]

    def link(sem, ref, target):
        return pltpu.make_async_remote_copy(ref, ref, sent.at[0], sem, device_id=(target,), device_id_type=MESH)

    def pair(sem, ref):
        return pltpu.make_async_remote_copy(ref, ref, sent.at[1], sem, device_id=(mate,), device_id_type=MESH)

    def settle(sem, ref):
        pltpu.make_async_copy(ref, ref, sem).wait()

    shift = lax.rem(me, 2) * depth

    def three(j, n=1):
        return b_all.at[pl.ds(j, n), pl.ds(pl.multiple_of(shift, depth), 3 * depth), :]

    def across(lo, hi, device):
        return b_all.at[pl.ds(lo, hi - lo), pl.ds(pl.multiple_of(device * depth, depth), depth), :]

    def a_copy(i):
        cols = chip_rows(order[i])
        group = 0 if i == 0 else 1 if i < 4 else 2
        return pltpu.make_async_copy(a_hbm.at[:, cols], a_all.at[:, cols], a_sem.at[group])

    def a_wait(lo, hi):
        width = (hi - lo) * 2 * depth
        settle(a_sem.at[0 if lo == 0 else 1 if lo == 1 else 2], a_all.at[:, pl.ds(pl.multiple_of(shift, depth), width)])

    def own_copy(j):
        return pltpu.make_async_copy(b_hbm.at[:, pl.ds(j * wide, wide)], b_all.at[j, pl.ds(pl.multiple_of(me * depth, depth), depth), :], own_sem)

    for j in range(CHUNKS):
        own_copy(j).start()
    a_copy(0).start()

    barrier = pltpu.get_barrier_semaphore()
    for device in (mate, *near):
        pl.semaphore_signal(barrier, inc=1, device_id=(device,), device_id_type=MESH)
    pl.semaphore_wait(barrier, 4)

    settle(own_sem, across(0, CHUNKS, me))
    for group, (lo, hi) in enumerate(((0, EARLY), (EARLY, CHUNKS))):
        pair(pair_own.at[group], across(lo, hi, me)).start()
    for u, (j, n) in enumerate(NEAR):
        for kind in range(3):
            link(near_sem.at[u], block(j, me, n), near[kind]).start()
    for i in range(1, 4):
        a_copy(i).start()

    def serve_near(u):
        j, n = NEAR[u]
        settle(near_sem.at[u], three(j, n))
        for kind, d in enumerate((2, 0, 1)):
            link(diag_sem.at[j // 2], block(j, near[kind], n), near[d]).start()
        for kind in range(3):
            pair(pair_near.at[u], block(j, near[kind], n)).start()

    part_rows = ((48, 48, 32), (32, 48, 48), (48, 32, 48))

    def serve_diag(u):
        settle(diag_sem.at[u], three(2 * u, 2))
        start = 0
        for d, count in enumerate(part_rows[u % 3]):
            source, target = ((dev_xy, dev_z), (dev_yz, dev_x), (dev_zx, dev_y))[d]
            link(far_sem, block(2 * u, source, 2, start, count), target).start()
            start += count
        for kind in range(3):
            pair(pair_diag.at[u], block(2 * u, diag[kind], 2)).start()

    def serve_far():
        settle(far_sem, across(0, CHUNKS, dev_far))
        pair(pair_far, across(0, CHUNKS, dev_far)).start()

    def add(j, sources, first=False, count=1):
        for r in range(0, rows, SUB):
            rs = pl.ds(r, SUB)
            for c in range(count):
                total = None if first else acc[j + c, rs, :]
                for device in sources:
                    ks = chip_rows(device)
                    term = dot(a_all[rs, ks], b_all[j + c, ks, :])
                    total = term if total is None else total + term
                acc[j + c, rs, :] = total

    a_wait(0, 1)
    settle(pair_own.at[0], across(0, EARLY, mate))
    for j in range(EARLY):
        add(j, (me,), True)
    serve_near(0)
    for i in range(4, 8):
        a_copy(i).start()
    settle(pair_own.at[1], across(EARLY, CHUNKS, mate))
    for j in range(EARLY, CHUNKS):
        add(j, (me,), True)

    def got_near(u):
        settle(pair_near.at[u], three(*NEAR[u]))

    def got_diag(u):
        settle(pair_diag.at[u], three(2 * u, 2))

    def steps(phase, lo, hi, table, count=1):
        @pl.loop(0, (hi - lo) // count)
        def _(s):
            j = lo + s * count
            late = lax.div(j + phase * CHUNKS, CHUNKS)
            for k, parts in table.items():
                @pl.when(j == k)
                def _():
                    for part, *arg in parts:
                        part(*arg)
            add(j, [n + late * (d - n) for n, d in zip(near, diag)], False, count)

    a_wait(1, 4)
    steps(0, 0, 4, {0: ((serve_near, 1), (got_near, 0)), 1: ((serve_near, 2), (got_near, 1)), 2: ((serve_near, 3), (got_near, 2)), 3: ((serve_near, 4), (got_near, 3))})
    steps(0, 4, 6, {4: ((got_near, 4),), 5: ((serve_near, 5),)})
    steps(0, 6, 8, {6: ((serve_diag, 0), (got_near, 5))}, 2)
    a_wait(4, 8)
    steps(1, 0, 2, {0: ((serve_diag, 1), (got_diag, 0))}, 2)
    steps(1, 2, 3, {2: ((serve_diag, 2), (got_diag, 1))})
    steps(1, 3, 5, {3: ((serve_diag, 3), (got_diag, 2))}, 2)
    steps(1, 5, 6, {5: ((serve_far,),)})
    got_diag(3)
    settle(pair_far, across(0, CHUNKS, flip(dev_far, 1)))
    settle(sent.at[0], b_all.at[pl.ds(0, CHUNKS - 1), pl.ds(0, 8 * depth), :])
    settle(sent.at[1], b_all.at[:, pl.ds(0, 8 * depth), :])


def finish_kernel(*refs):
    pl.run_scoped(lambda *tiles: finish_body(tiles, *refs), *accumulators())


def finish_body(tiles, b_ref, a_ref, acc_ref, c_hbm, stage, sem):
    chunks, size, wide = b_ref.shape
    blocks = c_hbm.shape[0] // BLOCK
    count = chunks // UNITS
    depth = size // 8
    chip = lax.div(lax.axis_index("fsdp"), 2)
    far = 7 - chip
    chips = (far, flip(far, 1), flip(far, 2), flip(far, 4))

    def part(device):
        return pl.ds(pl.multiple_of(device * depth, depth), depth)

    halves = BLOCK // TILE

    def rows_of(b, h=0, size=TILE):
        return pl.ds(pl.multiple_of(b * BLOCK + h * TILE, TILE), size)

    def put(b):
        slot = lax.rem(b, SLOTS)
        return pltpu.make_async_copy(stage.at[slot], c_hbm.at[rows_of(b, 0, BLOCK), :], sem.at[slot])

    def put_half(b, h):
        source = stage.at[b % SLOTS, pl.ds(h * TILE, TILE), :]
        return pltpu.make_async_copy(source, c_hbm.at[rows_of(b, h), :], sem.at[b % SLOTS if h == 0 else SLOTS])

    def keep(b, slot, t):
        h, i = divmod(t, count)
        for q in range(UNITS):
            j = UNITS * i + q
            total = acc_ref[j, rows_of(b, h), :] + result(tiles, t, q)
            stage[slot, pl.ds(h * TILE, TILE), j * wide:(j + 1) * wide] = total.astype(stage.dtype)

    passes = [(h * count + i, d) for h in range(halves) for i in range(count) for d in chips[:1 if UNITS * i < chunks - LEFT else 4]]
    every = halves * count

    def right(n, q):
        t, d = passes[n]
        return b_ref[UNITS * (t % count) + q, part(d), :]

    stage_right(right, 0)

    def work(b, start=True, wait=True, final=False):
        before = b - 1 if start else 0
        for n, (t, d) in enumerate(passes):
            if n + 1 < len(passes):
                stage_right(right, n + 1)
            for q in range(UNITS):
                pltpu.matmul_acc_lhs(tiles[q * RING + t % RING], a_ref[rows_of(b, t // count), part(d)], load_staged_rhs=n % 2)
            if n + 1 == len(passes):
                if not final:
                    stage_right(right, 0)
            elif passes[n + 1][0] == t:
                continue
            if t < LAG:
                keep(before, lax.rem(b + SLOTS - 1, SLOTS), every - LAG + t)
            else:
                keep(b, lax.rem(b, SLOTS), t - LAG)
            if t == LAG - 1:
                if start:
                    put(b - 1).start()
                if wait:
                    put(b - SLOTS).wait()
            if final and t == count + LAG - 1:
                put_half(b, 0).start()

    last = blocks - 1
    work(0, False, False)
    pl.loop(1, SLOTS)(lambda b: work(b, True, False))
    pl.loop(SLOTS, last)(work)
    work(last, True, True, True)
    for t in range(every - LAG, every):
        keep(last, last % SLOTS, t)
    put_half(last, 1).start()
    for b in range(blocks - SLOTS, last):
        put(b).wait()
    for h in range(halves):
        put_half(last, h).wait()


def solution(mesh):
    def local(a, b):
        rows, size = a.shape
        depth, cols = b.shape
        wide = cols // CHUNKS
        vmem = pl.BlockSpec(memory_space=pltpu.VMEM)
        hbm = pl.BlockSpec(memory_space=pl.ANY)
        dma = pltpu.SemaphoreType.DMA
        parts = pl.pallas_call(
            gather_kernel,
            out_shape=(
                pltpu.VMEM((CHUNKS, size, wide), jnp.bfloat16),
                pltpu.VMEM((rows, size), jnp.bfloat16),
                pltpu.VMEM((CHUNKS, rows, wide), jnp.float32),
            ),
            in_specs=[hbm, hbm],
            out_specs=(vmem, vmem, vmem),
            scratch_shapes=[
                dma((3,)), dma, dma((2,)),
                dma((len(NEAR),)), dma((CHUNKS // 2,)), dma,
                dma((2,)), dma((len(NEAR),)), dma((CHUNKS // 2,)), dma,
            ],
            compiler_params=pltpu.CompilerParams(collective_id=0, has_side_effects=True, vmem_limit_bytes=7 << 20),
            name="gather",
        )(a, pltpu.with_memory_space_constraint(b, pltpu.HBM))
        return pl.pallas_call(
            finish_kernel,
            out_shape=jax.ShapeDtypeStruct((rows, cols), jnp.bfloat16),
            in_specs=[vmem, vmem, vmem],
            out_specs=hbm,
            scratch_shapes=[pltpu.VMEM((SLOTS, BLOCK, cols), jnp.bfloat16), dma((SLOTS + 1,))],
            compiler_params=pltpu.CompilerParams(vmem_limit_bytes=15 << 19),
            name="finish",
        )(*(pltpu.with_memory_space_constraint(v, pltpu.VMEM) for v in parts))

    spec = P("fsdp", None)
    return jax.shard_map(local, mesh=mesh, in_specs=(spec, spec), out_specs=spec, check_vma=False)
```
